8 devices in a mesh: rep: 1 (over z), pp: 8 (over x, y, core).
Axes of the slice: x: 2, y: 2, z: 1, core: 2. Of those that a mesh axis runs over, the one named last changes fastest.
Arguments:
- x: bfloat16 [16, 512, 512], P('rep')
- dy: bfloat16 [16, 512, 512], P('rep')
- w_gate: bfloat16 [8, 512, 1408], P('pp')
- w_up: bfloat16 [8, 512, 1408], P('pp')
- w_down: bfloat16 [8, 1408, 512], P('pp')
Outputs:
- output 1: bfloat16 [8, 512, 1408], P(('rep', 'pp'))
- output 2: bfloat16 [8, 512, 1408], P(('rep', 'pp'))
- output 3: bfloat16 [8, 1408, 512], P(('rep', 'pp'))
All inputs are finite; a program needn't handle non-finite values.
Results may differ from the reference program's by a relative error of at most 0.0253.
Values are sent between devices in bfloat16 or wider.
A program may use at most 2 GiB of HBM per device.

```python
import jax
import jax.numpy as jnp
from jax import lax

MICRO = 16
TOKENS = 512
D = 512
FF = 1408
LAYERS = 8
NAMES = ("w_gate", "w_up", "w_down")
SHAPES = {"w_gate": (LAYERS, D, FF), "w_up": (LAYERS, D, FF), "w_down": (LAYERS, FF, D)}


def bump(key, n, height):
    away = (jnp.arange(n, dtype=jnp.int32) - jax.random.randint(key, (), 0, n, jnp.int32)) % n
    return jnp.where(away < n // 8, height, 1.0)


def together(key, own, strength):
    shared = jax.random.normal(key, own.shape[1:], jnp.float32)
    return (own + strength * shared) * lax.rsqrt(1 + strength * strength)


def setup_inputs(seed: int = 0, part: int = 0) -> dict:
    kx, kdy, ka, kb, kz, kf, kh, kl, *kw = jax.random.split(jax.random.key(seed), 8 + len(NAMES))
    kx, kdy, ka, kb = (jax.random.fold_in(k, part) for k in (kx, kdy, ka, kb))
    shape = (MICRO, TOKENS, D)
    much_x, much_dy = jax.random.uniform(kz, (2,), jnp.float32, 0.0, 1.0)
    layers = 2.0 ** jax.random.uniform(kl, (LAYERS, 1, 1), jnp.float32, -1.0, 1.0)
    x = together(ka, jax.random.normal(kx, shape, jnp.float32), much_x) * bump(kf, D, 4.0)
    dy = together(kb, jax.random.normal(kdy, shape, jnp.float32), much_dy)
    drawn = {"x": x.astype(jnp.bfloat16), "dy": (dy * (MICRO * TOKENS) ** -0.5).astype(jnp.bfloat16)}
    for key, name in zip(kw, NAMES, strict=True):
        w = jax.random.normal(key, SHAPES[name], jnp.float32) * SHAPES[name][1] ** -0.5
        drawn[name] = (w * {"w_gate": 1.0, "w_up": bump(kh, FF, 4.0), "w_down": layers}[name]).astype(jnp.bfloat16)
    return drawn


def matmul(a, w):
    return jnp.dot(a, w, preferred_element_type=jnp.float32).astype(jnp.bfloat16)


def normed(h):
    wide = h.astype(jnp.float32)
    scale = lax.rsqrt(jnp.mean(wide**2, -1, keepdims=True) + 1e-6)
    return (wide * scale).astype(jnp.bfloat16)


def layer(h, w):
    a = normed(h)
    gate = jnp.dot(a, w["w_gate"], preferred_element_type=jnp.float32)
    up = jnp.dot(a, w["w_up"], preferred_element_type=jnp.float32)
    return h + matmul((jax.nn.silu(gate) * up).astype(jnp.bfloat16), w["w_down"])


def stack(weights, h):
    return lax.scan(lambda h, w: (layer(h, w), None), h, weights)[0]


def reference(x, dy, w_gate, w_up, w_down):
    weights = dict(zip(NAMES, (w_gate, w_up, w_down), strict=True))

    def take(so_far, one):
        h, by_y = one
        _, back = jax.vjp(lambda w: stack(w, h), weights)
        return jax.tree.map(lambda total, term: total + term.astype(jnp.float32), so_far, back(by_y)[0]), None

    none_yet = {name: jnp.zeros(w.shape, jnp.float32) for name, w in weights.items()}
    by_weights, _ = lax.scan(take, none_yet, (x, dy))
    return tuple(by_weights[name].astype(jnp.bfloat16) for name in NAMES)
```

```python
import jax
import jax.numpy as jnp
from jax import lax
from jax.experimental import pallas as pl
from jax.experimental.pallas import tpu as pltpu
from jax.sharding import PartitionSpec as P

F32, BF16 = jnp.float32, jnp.bfloat16
ROWS = 256
RING = 4
EPS = 1e-6
AHEAD = (16, 16, 16, 16, 16, 16, 16, 0)


def dot(a, b):
    return jnp.dot(a, b, preferred_element_type=F32)


def kernel(
    x, dy, w_gate, w_up, w_down, o_gate, o_up, o_down,
    f_in, b_in, f_out, b_out, w_both, w_d, wt_d, wt_g, wt_u, acc_both, acc_d, a_t, hid, hid_t, d_both,
    f_recv, b_recv, f_send, b_send, w_sem, o_sem,
):
    micro, tokens, d = x.shape
    ff = w_down.shape[0]
    parts = tokens // ROWS
    blocks = ff // 128
    me = lax.axis_index("pp")
    stages = 8
    first, last = me == 0, me == stages - 1

    def w_copies():
        for j in range(blocks):
            src = pl.ds(128 * j, 128)
            yield pltpu.make_async_copy(w_gate.at[:, src], w_both.at[:, pl.ds(256 * j, 128)], w_sem.at[0, j])
            yield pltpu.make_async_copy(w_up.at[:, src], w_both.at[:, pl.ds(256 * j + 128, 128)], w_sem.at[1, j])
        yield pltpu.make_async_copy(w_down, w_d, w_sem.at[0, blocks])

    def chunk(ref, c):
        return ref.at[c // parts, pl.ds(pl.multiple_of((c % parts) * ROWS, ROWS), ROWS)]

    def f_copy(c):
        return pltpu.make_async_remote_copy(
            f_out.at[c % RING], chunk(f_in, c), f_send.at[c % RING], f_recv.at[c], device_id={"pp": jnp.minimum(me + 1, stages - 1)}
        )

    def b_copy(c):
        return pltpu.make_async_remote_copy(
            b_out.at[c % RING], chunk(b_in, c), b_send.at[c % RING], b_recv.at[c], device_id={"pp": jnp.maximum(me - 1, 0)}
        )

    for copy in w_copies():
        copy.start()

    @pl.when(first)
    def _():
        @pl.loop(0, micro * parts)
        def _(c):
            pltpu.make_async_copy(chunk(x, c), chunk(f_in, c), f_recv.at[c]).start()

    @pl.when(last)
    def _():
        @pl.loop(0, micro * parts)
        def _(c):
            pltpu.make_async_copy(chunk(dy, c), chunk(b_in, c), b_recv.at[c]).start()

    barrier = pltpu.get_barrier_semaphore()
    for other in range(1, stages):
        pl.semaphore_signal(barrier, inc=1, device_id={"pp": lax.rem(me + other, stages)})
    acc_both[...] = jnp.zeros_like(acc_both)
    acc_d[...] = jnp.zeros_like(acc_d)
    pl.semaphore_wait(barrier, stages - 1)

    for copy in w_copies():
        copy.wait()

    def scale_of(wide):
        return lax.rsqrt(jnp.mean(wide * wide, -1, keepdims=True) + EPS)

    def forward(c):
        f_copy(c).wait_recv()
        h = chunk(f_in, c)[...]

        @pl.when(~last)
        def _():
            wide = h.astype(F32)
            a = (wide * scale_of(wide)).astype(BF16)
            for j in range(blocks):
                both = dot(a, w_both[:, 256 * j : 256 * j + 256])
                gate, up = both[:, :128], both[:, 128:]
                hid[:, 128 * j : 128 * j + 128] = (gate * jax.nn.sigmoid(gate) * up).astype(BF16)

            @pl.when(c >= RING)
            def _():
                f_copy(c - RING).wait_send()

            f_out[c % RING] = h + dot(hid[...], w_d[...]).astype(BF16)
            f_copy(c).start()

    def backward(c):
        b_copy(c).wait_recv()
        rows = pl.ds(pl.multiple_of((c % parts) * ROWS, ROWS), ROWS)
        by_y = chunk(b_in, c)[...]
        wide = chunk(f_in, c)[...].astype(F32)
        scale = scale_of(wide)
        a = (wide * scale).astype(BF16)
        a_t[:, rows] = a.T
        for j in range(0, blocks, 2):
            n = min(2, blocks - j)
            by_hid = dot(by_y, wt_d[:, 128 * j : 128 * (j + n)]).astype(BF16).astype(F32)
            for k in range(j, j + n):
                both = dot(a, w_both[:, 256 * k : 256 * k + 256])
                gate, up = both[:, :128], both[:, 128:]
                by = by_hid[:, 128 * (k - j) : 128 * (k - j) + 128]
                sig = jax.nn.sigmoid(gate)
                silu = gate * sig
                hid_t[128 * k : 128 * k + 128, rows] = (silu * up).astype(BF16).T
                d_both[rows, ff + 128 * k : ff + 128 * k + 128] = (by * silu).astype(BF16)
                by_silu = by * up
                d_both[rows, 128 * k : 128 * k + 128] = (by_silu * (sig + silu * (1 - sig))).astype(BF16)

        @pl.when(~first)
        def _():
            by_a = (dot(d_both[rows, :ff], wt_g[...]).astype(BF16) + dot(d_both[rows, ff:], wt_u[...]).astype(BF16)).astype(F32)
            wide = chunk(f_in, c)[...].astype(F32)
            scale = scale_of(wide)
            by_scale = jnp.sum(by_a * wide, -1, keepdims=True)
            by_wide = by_a * scale - wide * (by_scale * scale * scale * scale * (1.0 / d))

            @pl.when(c >= RING)
            def _():
                b_copy(c - RING).wait_send()

            b_out[c % RING] = chunk(b_in, c)[...] + by_wide.astype(BF16)
            b_copy(c).start()

    def by_weights(m):
        for j in range(2 * blocks // 2):
            cols = slice(256 * j, 256 * j + 256)
            acc_both[:, cols] += dot(a_t[...], d_both[:, cols]).astype(BF16).astype(F32)
        by_y = b_in[m]
        for j in range(0, ff, 352):
            rows = slice(j, j + 352)
            acc_d[rows, :] += dot(hid_t[rows, :], by_y).astype(BF16).astype(F32)

    ahead = jnp.int32(0)
    for s, k in enumerate(AHEAD):
        ahead = jnp.where(me == s, k, ahead)

    @pl.loop(0, micro + max(AHEAD))
    def _(i):
        @pl.when(i < micro)
        def _():
            @pl.loop(0, parts)
            def _(p):
                forward(parts * i + p)

        @pl.when(i == 0)
        def _():
            @pl.loop(0, blocks)
            def _(j):
                cols = pl.ds(pl.multiple_of(128 * j, 128), 128)
                wt_d[:, cols] = w_d[cols, :].T
                wt_g[cols, :] = w_both[:, pl.ds(pl.multiple_of(256 * j, 128), 128)].T
                wt_u[cols, :] = w_both[:, pl.ds(pl.multiple_of(256 * j + 128, 128), 128)].T

        m = i - ahead

        @pl.when((m >= 0) & (m < micro))
        def _():
            @pl.loop(0, parts)
            def _(p):
                backward(parts * m + p)

            by_weights(m)

    for c in range(micro * parts - RING, micro * parts):

        @pl.when(~last)
        def _():
            f_copy(c).wait_send()

        @pl.when(~first)
        def _():
            b_copy(c).wait_send()

    d_both[...] = acc_both[...].astype(BF16)
    hid_t[...] = acc_d[...].astype(BF16)
    out = (
        pltpu.make_async_copy(d_both.at[:, pl.ds(0, ff)], o_gate, o_sem.at[0]),
        pltpu.make_async_copy(d_both.at[:, pl.ds(ff, ff)], o_up, o_sem.at[1]),
        pltpu.make_async_copy(hid_t, o_down, o_sem.at[2]),
    )
    for copy in out:
        copy.start()
    for copy in out:
        copy.wait()


def solution(mesh):
    def step(x, dy, w_gate, w_up, w_down):
        micro, tokens, d = x.shape
        ff = w_down.shape[1]
        chunks = micro * tokens // ROWS
        hbm = pl.BlockSpec(memory_space=pl.ANY)
        dma = pltpu.SemaphoreType.DMA
        outs = pl.pallas_call(
            kernel,
            out_shape=tuple(jax.ShapeDtypeStruct(w.shape[1:], w.dtype) for w in (w_gate, w_up, w_down)),
            in_specs=[hbm] * 5,
            out_specs=(hbm,) * 3,
            scratch_shapes=[
                pltpu.VMEM((micro, tokens, d), BF16),
                pltpu.VMEM((micro, tokens, d), BF16),
                pltpu.VMEM((RING, ROWS, d), BF16),
                pltpu.VMEM((RING, ROWS, d), BF16),
                pltpu.VMEM((d, 2 * ff), BF16),
                pltpu.VMEM((ff, d), BF16),
                pltpu.VMEM((d, ff), BF16),
                pltpu.VMEM((ff, d), BF16),
                pltpu.VMEM((ff, d), BF16),
                pltpu.VMEM((d, 2 * ff), F32),
                pltpu.VMEM((ff, d), F32),
                pltpu.VMEM((d, tokens), BF16),
                pltpu.VMEM((ROWS, ff), BF16),
                pltpu.VMEM((ff, tokens), BF16),
                pltpu.VMEM((tokens, 2 * ff), BF16),
                dma((chunks,)),
                dma((chunks,)),
                dma((RING,)),
                dma((RING,)),
                dma((2, ff // 128 + 1)),
                dma((3,)),
            ],
            compiler_params=pltpu.CompilerParams(
                collective_id=0, has_side_effects=True, vmem_limit_bytes=60 * 1024 * 1024
            ),
        )(x, dy, w_gate[0], w_up[0], w_down[0])
        return tuple(o[None] for o in outs)

    return jax.shard_map(
        step,
        mesh=mesh,
        in_specs=(P("rep", None, None),) * 2 + (P("pp", None, None),) * 3,
        out_specs=(P(("rep", "pp"), None, None),) * 3,
        check_vma=False,
    )
```

```python
import jax
import jax.numpy as jnp
from jax import lax
from jax.experimental import pallas as pl
from jax.experimental.pallas import tpu as pltpu
from jax.sharding import PartitionSpec as P

F32, BF16 = jnp.float32, jnp.bfloat16
ROWS = 256
RING = 4
EPS = 1e-6
AHEAD = (14, 13, 11, 10, 6, 5, 2, 0)


def dot(a, b):
    return jnp.dot(a, b, preferred_element_type=F32)


def kernel(
    x, dy, w_gate, w_up, w_down, o_gate, o_up, o_down, kept_pq, kept_hid,
    f_in, b_in, f_out, b_out, w_both, w_d, wt_d, wt_g, wt_u, acc_both, acc_d, a_t, hid_t, d_both, pq_out, hid_out, pq_in, hid_in,
    f_recv, b_recv, f_send, b_send, w_sem, o_sem, out_sem, in_sem,
):
    micro, tokens, d = x.shape
    ff = w_down.shape[0]
    parts = tokens // ROWS
    blocks = ff // 128
    me = lax.axis_index("pp")
    stages = 8
    first, last = me == 0, me == stages - 1

    def w_copies():
        for j in range(blocks):
            src = pl.ds(128 * j, 128)
            yield pltpu.make_async_copy(w_gate.at[:, src], w_both.at[:, pl.ds(256 * j, 128)], w_sem.at[0, j])
            yield pltpu.make_async_copy(w_up.at[:, src], w_both.at[:, pl.ds(256 * j + 128, 128)], w_sem.at[1, j])
        yield pltpu.make_async_copy(w_down, w_d, w_sem.at[0, blocks])

    def chunk(ref, c):
        return ref.at[c // parts, pl.ds(pl.multiple_of((c % parts) * ROWS, ROWS), ROWS)]

    def f_copy(c):
        return pltpu.make_async_remote_copy(
            f_out.at[c % RING], chunk(f_in, c), f_send.at[c % RING], f_recv.at[c], device_id={"pp": jnp.minimum(me + 1, stages - 1)}
        )

    def b_copy(c):
        return pltpu.make_async_remote_copy(
            b_out.at[c % RING], chunk(b_in, c), b_send.at[c % RING], b_recv.at[c], device_id={"pp": jnp.maximum(me - 1, 0)}
        )

    def kept_out(c):
        slot = c % 2
        return (
            pltpu.make_async_copy(pq_out.at[slot], kept_pq.at[c], out_sem.at[0, slot]),
            pltpu.make_async_copy(hid_out.at[slot], kept_hid.at[c], out_sem.at[1, slot]),
        )

    def kept_in(c):
        slot = c % 2
        return (
            pltpu.make_async_copy(kept_pq.at[c], pq_in.at[slot], in_sem.at[0, slot]),
            pltpu.make_async_copy(kept_hid.at[c], hid_in.at[slot], in_sem.at[1, slot]),
        )

    for copy in w_copies():
        copy.start()

    @pl.when(first)
    def _():
        @pl.loop(0, micro * parts)
        def _(c):
            pltpu.make_async_copy(chunk(x, c), chunk(f_in, c), f_recv.at[c]).start()

    @pl.when(last)
    def _():
        @pl.loop(0, micro * parts)
        def _(c):
            pltpu.make_async_copy(chunk(dy, c), chunk(b_in, c), b_recv.at[c]).start()

    barrier = pltpu.get_barrier_semaphore()
    for other in range(1, stages):
        pl.semaphore_signal(barrier, inc=1, device_id={"pp": lax.rem(me + other, stages)})
    acc_both[...] = jnp.zeros_like(acc_both)
    acc_d[...] = jnp.zeros_like(acc_d)
    pl.semaphore_wait(barrier, stages - 1)

    for copy in w_copies():
        copy.wait()

    def scale_of(wide):
        return lax.rsqrt(jnp.mean(wide * wide, -1, keepdims=True) + EPS)

    def gates(both):
        gate, up = both[:, :128], both[:, 128:]
        sig = jax.nn.sigmoid(gate)
        silu = gate * sig
        return silu, up * (sig + silu * (1 - sig)), (silu * up).astype(BF16)

    def forward(c):
        f_copy(c).wait_recv()

        @pl.when(~last)
        def _():
            slot = c % 2

            @pl.when(c >= 2)
            def _():
                for copy in kept_out(c - 2):
                    copy.wait()

            @pl.when(c >= RING)
            def _():
                f_copy(c - RING).wait_send()

            h = chunk(f_in, c)[...]
            wide = h.astype(F32)
            a = (wide * scale_of(wide)).astype(BF16)
            for j in range(blocks):
                silu, by_gate, hid = gates(dot(a, w_both[:, 256 * j : 256 * j + 256]))
                pq_out[slot, :, 256 * j : 256 * j + 128] = silu
                pq_out[slot, :, 256 * j + 128 : 256 * j + 256] = by_gate
                hid_out[slot, :, 128 * j : 128 * j + 128] = hid
            f_out[c % RING] = h + dot(hid_out[slot], w_d[...]).astype(BF16)
            f_copy(c).start()
            for copy in kept_out(c):
                copy.start()

    def rows_of(c):
        return pl.ds(pl.multiple_of((c % parts) * ROWS, ROWS), ROWS)

    def backward_last(c):
        b_copy(c).wait_recv()
        rows = rows_of(c)
        by_y = chunk(b_in, c)[...]
        wide = chunk(f_in, c)[...].astype(F32)
        a = (wide * scale_of(wide)).astype(BF16)
        a_t[:, rows] = a.T
        for j in range(0, blocks, 2):
            n = min(2, blocks - j)
            by_hid = dot(by_y, wt_d[:, 128 * j : 128 * (j + n)]).astype(BF16).astype(F32)
            for k in range(j, j + n):
                silu, by_gate, hid = gates(dot(a, w_both[:, 256 * k : 256 * k + 256]))
                by = by_hid[:, 128 * (k - j) : 128 * (k - j) + 128]
                hid_t[128 * k : 128 * k + 128, rows] = hid.T
                d_both[rows, 128 * k : 128 * k + 128] = (by * by_gate).astype(BF16)
                d_both[rows, ff + 128 * k : ff + 128 * k + 128] = (by * silu).astype(BF16)
        send_back(c)

    def backward(c):
        @pl.when(c + 1 < micro * parts)
        def _():
            for copy in kept_in(c + 1):
                copy.start()

        for copy in kept_in(c):
            copy.wait()
        b_copy(c).wait_recv()
        slot = c % 2
        rows = rows_of(c)
        by_y = chunk(b_in, c)[...]
        wide = chunk(f_in, c)[...].astype(F32)
        a_t[:, rows] = (wide * scale_of(wide)).astype(BF16).T
        hid_t[:, rows] = hid_in[slot].T
        for j in range(0, blocks, 2):
            n = min(2, blocks - j)
            by_hid = dot(by_y, wt_d[:, 128 * j : 128 * (j + n)]).astype(BF16).astype(F32)
            for k in range(j, j + n):
                by = by_hid[:, 128 * (k - j) : 128 * (k - j) + 128]
                d_both[rows, 128 * k : 128 * k + 128] = (by * pq_in[slot, :, 256 * k + 128 : 256 * k + 256]).astype(BF16)
                d_both[rows, ff + 128 * k : ff + 128 * k + 128] = (by * pq_in[slot, :, 256 * k : 256 * k + 128]).astype(BF16)

        @pl.when(~first)
        def _():
            send_back(c)

    def send_back(c):
        @pl.when(c >= RING)
        def _():
            b_copy(c - RING).wait_send()

        rows = rows_of(c)
        wide = chunk(f_in, c)[...].astype(F32)
        scale = scale_of(wide)
        by_a = (dot(d_both[rows, :ff], wt_g[...]).astype(BF16) + dot(d_both[rows, ff:], wt_u[...]).astype(BF16)).astype(F32)
        by_scale = jnp.sum(by_a * wide, -1, keepdims=True)
        by_wide = by_a * scale - wide * (by_scale * scale * scale * scale * (1.0 / d))
        b_out[c % RING] = chunk(b_in, c)[...] + by_wide.astype(BF16)
        b_copy(c).start()

    def by_weights(m):
        for j in range(2 * blocks // 2):
            cols = slice(256 * j, 256 * j + 256)
            acc_both[:, cols] += dot(a_t[...], d_both[:, cols]).astype(BF16).astype(F32)
        by_y = b_in[m]
        for j in range(0, ff, 352):
            rows = slice(j, j + 352)
            acc_d[rows, :] += dot(hid_t[rows, :], by_y).astype(BF16).astype(F32)

    ahead = jnp.int32(0)
    for s, k in enumerate(AHEAD):
        ahead = jnp.where(me == s, k, ahead)

    @pl.loop(0, micro + max(AHEAD))
    def _(i):
        @pl.when(i < micro)
        def _():
            @pl.loop(0, parts)
            def _(p):
                forward(parts * i + p)

        @pl.when(i == 0)
        def _():
            @pl.loop(0, blocks)
            def _(j):
                cols = pl.ds(pl.multiple_of(128 * j, 128), 128)
                wt_d[:, cols] = w_d[cols, :].T
                wt_g[cols, :] = w_both[:, pl.ds(pl.multiple_of(256 * j, 128), 128)].T
                wt_u[cols, :] = w_both[:, pl.ds(pl.multiple_of(256 * j + 128, 128), 128)].T

        @pl.when((i == micro) & ~last)
        def _():
            for c in range(micro * parts - 2, micro * parts):
                for copy in kept_out(c):
                    copy.wait()

        @pl.when((i == ahead - 1) & ~last)
        def _():
            for copy in kept_in(0):
                copy.start()

        m = i - ahead

        @pl.when((m >= 0) & (m < micro))
        def _():
            @pl.loop(0, parts)
            def _(p):
                @pl.when(last)
                def _():
                    backward_last(parts * m + p)

                @pl.when(~last)
                def _():
                    backward(parts * m + p)

            by_weights(m)

    for c in range(micro * parts - RING, micro * parts):

        @pl.when(~last)
        def _():
            f_copy(c).wait_send()

        @pl.when(~first)
        def _():
            b_copy(c).wait_send()

    d_both[...] = acc_both[...].astype(BF16)
    hid_t[...] = acc_d[...].astype(BF16)
    out = (
        pltpu.make_async_copy(d_both.at[:, pl.ds(0, ff)], o_gate, o_sem.at[0]),
        pltpu.make_async_copy(d_both.at[:, pl.ds(ff, ff)], o_up, o_sem.at[1]),
        pltpu.make_async_copy(hid_t, o_down, o_sem.at[2]),
    )
    for copy in out:
        copy.start()
    for copy in out:
        copy.wait()


def solution(mesh):
    def step(x, dy, w_gate, w_up, w_down):
        micro, tokens, d = x.shape
        ff = w_down.shape[1]
        chunks = micro * tokens // ROWS
        hbm = pl.BlockSpec(memory_space=pl.ANY)
        dma = pltpu.SemaphoreType.DMA
        outs = pl.pallas_call(
            kernel,
            out_shape=(
                *(jax.ShapeDtypeStruct(w.shape[1:], w.dtype) for w in (w_gate, w_up, w_down)),
                jax.ShapeDtypeStruct((chunks, ROWS, 2 * ff), F32),
                jax.ShapeDtypeStruct((chunks, ROWS, ff), BF16),
            ),
            in_specs=[hbm] * 5,
            out_specs=(hbm,) * 5,
            scratch_shapes=[
                pltpu.VMEM((micro, tokens, d), BF16),
                pltpu.VMEM((micro, tokens, d), BF16),
                pltpu.VMEM((RING, ROWS, d), BF16),
                pltpu.VMEM((RING, ROWS, d), BF16),
                pltpu.VMEM((d, 2 * ff), BF16),
                pltpu.VMEM((ff, d), BF16),
                pltpu.VMEM((d, ff), BF16),
                pltpu.VMEM((ff, d), BF16),
                pltpu.VMEM((ff, d), BF16),
                pltpu.VMEM((d, 2 * ff), F32),
                pltpu.VMEM((ff, d), F32),
                pltpu.VMEM((d, tokens), BF16),
                pltpu.VMEM((ff, tokens), BF16),
                pltpu.VMEM((tokens, 2 * ff), BF16),
                pltpu.VMEM((2, ROWS, 2 * ff), F32),
                pltpu.VMEM((2, ROWS, ff), BF16),
                pltpu.VMEM((2, ROWS, 2 * ff), F32),
                pltpu.VMEM((2, ROWS, ff), BF16),
                dma((chunks,)),
                dma((chunks,)),
                dma((RING,)),
                dma((RING,)),
                dma((2, ff // 128 + 1)),
                dma((3,)),
                dma((2, 2)),
                dma((2, 2)),
            ],
            compiler_params=pltpu.CompilerParams(
                collective_id=0, has_side_effects=True, vmem_limit_bytes=67_043_328
            ),
        )(x, dy, w_gate[0], w_up[0], w_down[0])
        return tuple(o[None] for o in outs[:3])

    return jax.shard_map(
        step,
        mesh=mesh,
        in_specs=(P("rep", None, None),) * 2 + (P("pp", None, None),) * 3,
        out_specs=(P(("rep", "pp"), None, None),) * 3,
        check_vma=False,
    )
```

```python
import jax
import jax.numpy as jnp
from jax import lax
from jax.experimental import pallas as pl
from jax.experimental.pallas import tpu as pltpu
from jax.sharding import PartitionSpec as P

F32, BF16 = jnp.float32, jnp.bfloat16
EPS = 1e-6
Q = 128
COARSE, FINE = 256, 128
AHEAD = (14, 13, 10, 9, 6, 5, 2, 0)
FINE_F = 6
FINE_B = 6
FINE_E = 6
RELAY_F, RELAY_B = 0, 7
LAG_F = 3
LAG_B = 3


def dot(a, b):
    return jnp.dot(a, b, preferred_element_type=F32)


def kernel(
    x, dy, w_gate, w_up, w_down, o_gate, o_up, o_down, kept_pq, kept_hid,
    f_in, b_in, r_in, f_out, b_out, w_both, w_d, wt_d, wt_g, wt_u, acc_both, acc_d, a_t, hid_t, d_both, pq_out, hid_out, pq_in, hid_in,
    f_recv, b_recv, r_recv, f_send, b_send, r_send, w_sem, o_sem, out_sem, in_sem,
):
    micro, tokens, d = x.shape
    ff = w_down.shape[0]
    quarters = tokens // Q
    blocks = ff // 128
    me = lax.axis_index("pp")
    stages = 8
    first, last = me == 0, me == stages - 1

    def w_copies():
        for j in range(blocks):
            src = pl.ds(128 * j, 128)
            yield pltpu.make_async_copy(w_gate.at[:, src], w_both.at[:, pl.ds(256 * j, 128)], w_sem.at[0, j])
            yield pltpu.make_async_copy(w_up.at[:, src], w_both.at[:, pl.ds(256 * j + 128, 128)], w_sem.at[1, j])
        yield pltpu.make_async_copy(w_down, w_d, w_sem.at[0, blocks])

    def rows(q, n=Q):
        return pl.ds(pl.multiple_of(q * Q, Q), n)

    def f_copy(m, q, to=None):
        to = jnp.minimum(me + 1, stages - 1) if to is None else to
        return pltpu.make_async_remote_copy(
            f_out.at[m % 2, rows(q)], f_in.at[m, rows(q)], f_send.at[m % 2, q], f_recv.at[m, q], device_id={"pp": to}
        )

    def b_copy(m, q, to=None):
        to = jnp.maximum(me - 1, 0) if to is None else to
        return pltpu.make_async_remote_copy(
            b_out.at[m % 2, rows(q)], b_in.at[m, rows(q)], b_send.at[m % 2, q], b_recv.at[m, q], device_id={"pp": to}
        )

    def f_by_relay(m, q):
        return pltpu.make_async_remote_copy(
            f_out.at[m % 2, rows(q)], r_in.at[m, q // 2], f_send.at[m % 2, q], r_recv.at[m, q // 2], device_id={"pp": RELAY_F}
        )

    def b_by_relay(m, q):
        return pltpu.make_async_remote_copy(
            b_out.at[m % 2, rows(q)], r_in.at[m, q // 2], b_send.at[m % 2, q], r_recv.at[m, q // 2], device_id={"pp": RELAY_B}
        )

    def f_relay(m, q):
        return pltpu.make_async_remote_copy(
            r_in.at[m, q // 2], f_in.at[m, rows(q)], r_send.at[m, q // 2], f_recv.at[m, q], device_id={"pp": 4}
        )

    def b_relay(m, q):
        return pltpu.make_async_remote_copy(
            r_in.at[m, q // 2], b_in.at[m, rows(q)], r_send.at[m, q // 2], b_recv.at[m, q], device_id={"pp": 3}
        )

    def send(m, q, nq, hop, copy, by_relay):
        for k in range(nq):

            @pl.when((me == hop) & ((q + k) % 2 == 0))
            def _():
                by_relay(m, q + k).start()

            @pl.when((me != hop) | ((q + k) % 2 == 1))
            def _():
                copy(m, q + k).start()

    def kept_out(m, q):
        return (
            pltpu.make_async_copy(pq_out.at[rows(q)], kept_pq.at[m, rows(q)], out_sem.at[0, q]),
            pltpu.make_async_copy(hid_out.at[rows(q)], kept_hid.at[m, rows(q)], out_sem.at[1, q]),
        )

    def kept_in(m, q):
        return (
            pltpu.make_async_copy(kept_pq.at[m, rows(q)], pq_in.at[rows(q)], in_sem.at[0, q]),
            pltpu.make_async_copy(kept_hid.at[m, rows(q)], hid_in.at[rows(q)], in_sem.at[1, q]),
        )

    for copy in w_copies():
        copy.start()

    def each(body):
        @pl.loop(0, micro)
        def _(m):
            @pl.loop(0, quarters)
            def _(q):
                body(m, q)

    @pl.when(first)
    def _():
        each(lambda m, q: pltpu.make_async_copy(x.at[m, rows(q)], f_in.at[m, rows(q)], f_recv.at[m, q]).start())

    @pl.when(last)
    def _():
        each(lambda m, q: pltpu.make_async_copy(dy.at[m, rows(q)], b_in.at[m, rows(q)], b_recv.at[m, q]).start())

    barrier = pltpu.get_barrier_semaphore()
    for other in range(1, stages):
        pl.semaphore_signal(barrier, inc=1, device_id={"pp": lax.rem(me + other, stages)})
    acc_both[...] = jnp.zeros_like(acc_both)
    acc_d[...] = jnp.zeros_like(acc_d)
    pl.semaphore_wait(barrier, stages - 1)

    for copy in w_copies():
        copy.wait()

    def scale_of(wide):
        return lax.rsqrt(jnp.mean(wide * wide, -1, keepdims=True) + EPS)

    def gates(both):
        gate, up = both[:, :128], both[:, 128:]
        sig = jax.nn.sigmoid(gate)
        silu = gate * sig
        return silu, up * (sig + silu * (1 - sig)), (silu * up).astype(BF16)

    def forward(m, q, n):
        nq = n // Q
        for k in range(nq):
            f_copy(m, q + k).wait_recv()

        @pl.when(~last)
        def _():
            @pl.when(m >= 1)
            def _():
                for k in range(nq):
                    for copy in kept_out(m - 1, q + k):
                        copy.wait()

            @pl.when(m >= 2)
            def _():
                for k in range(nq):
                    f_copy(m - 2, q + k).wait_send()

            here = rows(q, n)
            h = f_in[m, here]
            wide = h.astype(F32)
            a = (wide * scale_of(wide)).astype(BF16)
            for j in range(blocks):
                silu, by_gate, hid = gates(dot(a, w_both[:, 256 * j : 256 * j + 256]))
                pq_out[here, 256 * j : 256 * j + 128] = silu
                pq_out[here, 256 * j + 128 : 256 * j + 256] = by_gate
                hid_out[here, 128 * j : 128 * j + 128] = hid
            f_out[m % 2, here] = h + dot(hid_out[here], w_d[...]).astype(BF16)
            send(m, q, nq, 3, f_copy, f_by_relay)
            for k in range(nq):
                for copy in kept_out(m, q + k):
                    copy.start()

    def send_back(m, q, n):
        nq = n // Q

        @pl.when(m >= 2)
        def _():
            for k in range(nq):
                b_copy(m - 2, q + k).wait_send()

        here = rows(q, n)
        wide = f_in[m, here].astype(F32)
        scale = scale_of(wide)
        by_a = (dot(d_both[here, :ff], wt_g[...]).astype(BF16) + dot(d_both[here, ff:], wt_u[...]).astype(BF16)).astype(F32)
        by_scale = jnp.sum(by_a * wide, -1, keepdims=True)
        by_wide = by_a * scale - wide * (by_scale * scale * scale * scale * (1.0 / d))
        b_out[m % 2, here] = b_in[m, here] + by_wide.astype(BF16)
        send(m, q, nq, 4, b_copy, b_by_relay)

    def backward_last(m, q, n):
        for k in range(n // Q):
            b_copy(m, q + k).wait_recv()
        here = rows(q, n)
        by_y = b_in[m, here]
        wide = f_in[m, here].astype(F32)
        a = (wide * scale_of(wide)).astype(BF16)
        a_t[:, here] = a.T
        for j in range(0, blocks, 2):
            c = min(2, blocks - j)
            by_hid = dot(by_y, wt_d[:, 128 * j : 128 * (j + c)]).astype(BF16).astype(F32)
            for k in range(j, j + c):
                silu, by_gate, hid = gates(dot(a, w_both[:, 256 * k : 256 * k + 256]))
                by = by_hid[:, 128 * (k - j) : 128 * (k - j) + 128]
                hid_t[128 * k : 128 * k + 128, here] = hid.T
                d_both[here, 128 * k : 128 * k + 128] = (by * by_gate).astype(BF16)
                d_both[here, ff + 128 * k : ff + 128 * k + 128] = (by * silu).astype(BF16)
        send_back(m, q, n)

    def backward(m, q, n):
        nq = n // Q
        for k in range(nq):
            ahead_m, ahead_q = m + (q + k + 2) // quarters, (q + k + 2) % quarters

            @pl.when(ahead_m < micro)
            def _():
                for copy in kept_in(ahead_m, ahead_q):
                    copy.start()

        for k in range(nq):
            for copy in kept_in(m, q + k):
                copy.wait()
            b_copy(m, q + k).wait_recv()
        here = rows(q, n)
        by_y = b_in[m, here]
        wide = f_in[m, here].astype(F32)
        a_t[:, here] = (wide * scale_of(wide)).astype(BF16).T
        hid_t[:, here] = hid_in[here].T
        for j in range(0, blocks, 2):
            c = min(2, blocks - j)
            by_hid = dot(by_y, wt_d[:, 128 * j : 128 * (j + c)]).astype(BF16).astype(F32)
            for k in range(j, j + c):
                by = by_hid[:, 128 * (k - j) : 128 * (k - j) + 128]
                d_both[here, 128 * k : 128 * k + 128] = (by * pq_in[here, 256 * k + 128 : 256 * k + 256]).astype(BF16)
                d_both[here, ff + 128 * k : ff + 128 * k + 128] = (by * pq_in[here, 256 * k : 256 * k + 128]).astype(BF16)

        @pl.when(~first)
        def _():
            send_back(m, q, n)

    def by_weights(m):
        for j in range(blocks):
            cols = slice(256 * j, 256 * j + 256)
            acc_both[:, cols] += dot(a_t[...], d_both[:, cols]).astype(BF16).astype(F32)
        by_y = b_in[m]
        for j in range(0, ff, 352):
            acc_d[j : j + 352, :] += dot(hid_t[j : j + 352, :], by_y).astype(BF16).astype(F32)

    def in_chunks(body, m, fine):
        for n, which in ((FINE, fine), (COARSE, ~fine)):

            @pl.when(which)
            def _():
                @pl.loop(0, tokens // n)
                def _(p):
                    body(m, p * (n // Q), n)

    ahead = jnp.int32(0)
    for s, k in enumerate(AHEAD):
        ahead = jnp.where(me == s, k, ahead)

    @pl.loop(0, micro + max(AHEAD))
    def _(i):
        @pl.when(i < micro)
        def _():
            in_chunks(forward, i, i < FINE_F)

        @pl.when(i == 0)
        def _():
            @pl.loop(0, blocks)
            def _(j):
                cols = pl.ds(pl.multiple_of(128 * j, 128), 128)
                wt_d[:, cols] = w_d[cols, :].T
                wt_g[cols, :] = w_both[:, pl.ds(pl.multiple_of(256 * j, 128), 128)].T
                wt_u[cols, :] = w_both[:, pl.ds(pl.multiple_of(256 * j + 128, 128), 128)].T

        @pl.when((i == micro) & ~last)
        def _():
            for q in range(quarters):
                for copy in kept_out(micro - 1, q):
                    copy.wait()

        @pl.when((i == ahead - 1) & ~last)
        def _():
            for q in range(2):
                for copy in kept_in(0, q):
                    copy.start()

        for device, lag, arrives, relay in ((RELAY_F, LAG_F, f_by_relay, f_relay), (RELAY_B, LAG_B, b_by_relay, b_relay)):

            @pl.when((me == device) & (i >= lag) & (i < micro + lag))
            def _():
                for q in range(0, quarters, 2):
                    arrives(i - lag, q).wait_recv()
                    relay(i - lag, q).start()

        m = i - ahead

        @pl.when((m >= 0) & (m < micro))
        def _():
            fine = (m < FINE_B) | (m >= micro - FINE_E)

            @pl.when(last)
            def _():
                in_chunks(backward_last, m, fine)

            @pl.when(~last)
            def _():
                in_chunks(backward, m, fine)

            by_weights(m)

    for m in range(micro - 2, micro):
        for q in range(quarters):

            @pl.when(~last)
            def _():
                f_copy(m, q).wait_send()

            @pl.when(~first)
            def _():
                b_copy(m, q).wait_send()

    for device, relay in ((RELAY_F, f_relay), (RELAY_B, b_relay)):

        @pl.when(me == device)
        def _():
            @pl.loop(0, micro)
            def _(m):
                for q in range(0, quarters, 2):
                    relay(m, q).wait_send()

    d_both[...] = acc_both[...].astype(BF16)
    hid_t[...] = acc_d[...].astype(BF16)
    out = (
        pltpu.make_async_copy(d_both.at[:, pl.ds(0, ff)], o_gate, o_sem.at[0]),
        pltpu.make_async_copy(d_both.at[:, pl.ds(ff, ff)], o_up, o_sem.at[1]),
        pltpu.make_async_copy(hid_t, o_down, o_sem.at[2]),
    )
    for copy in out:
        copy.start()
    for copy in out:
        copy.wait()


def solution(mesh):
    def step(x, dy, w_gate, w_up, w_down):
        micro, tokens, d = x.shape
        ff = w_down.shape[1]
        quarters = tokens // Q
        hbm = pl.BlockSpec(memory_space=pl.ANY)
        dma = pltpu.SemaphoreType.DMA
        outs = pl.pallas_call(
            kernel,
            out_shape=(
                *(jax.ShapeDtypeStruct(w.shape[1:], w.dtype) for w in (w_gate, w_up, w_down)),
                jax.ShapeDtypeStruct((micro, tokens, 2 * ff), F32),
                jax.ShapeDtypeStruct((micro, tokens, ff), BF16),
            ),
            in_specs=[hbm] * 5,
            out_specs=(hbm,) * 5,
            scratch_shapes=[
                pltpu.VMEM((micro, tokens, d), BF16),
                pltpu.VMEM((micro, tokens, d), BF16),
                pltpu.VMEM((micro, quarters // 2, Q, d), BF16),
                pltpu.VMEM((2, tokens, d), BF16),
                pltpu.VMEM((2, tokens, d), BF16),
                pltpu.VMEM((d, 2 * ff), BF16),
                pltpu.VMEM((ff, d), BF16),
                pltpu.VMEM((d, ff), BF16),
                pltpu.VMEM((ff, d), BF16),
                pltpu.VMEM((ff, d), BF16),
                pltpu.VMEM((d, 2 * ff), F32),
                pltpu.VMEM((ff, d), F32),
                pltpu.VMEM((d, tokens), BF16),
                pltpu.VMEM((ff, tokens), BF16),
                pltpu.VMEM((tokens, 2 * ff), BF16),
                pltpu.VMEM((tokens, 2 * ff), F32),
                pltpu.VMEM((tokens, ff), BF16),
                pltpu.VMEM((tokens, 2 * ff), F32),
                pltpu.VMEM((tokens, ff), BF16),
                dma((micro, quarters)),
                dma((micro, quarters)),
                dma((micro, quarters // 2)),
                dma((2, quarters)),
                dma((2, quarters)),
                dma((micro, quarters // 2)),
                dma((2, ff // 128 + 1)),
                dma((3,)),
                dma((2, quarters)),
                dma((2, quarters)),
            ],
            compiler_params=pltpu.CompilerParams(
                collective_id=0, has_side_effects=True, vmem_limit_bytes=67_043_328
            ),
        )(x, dy, w_gate[0], w_up[0], w_down[0])
        return tuple(o[None] for o in outs[:3])

    return jax.shard_map(
        step,
        mesh=mesh,
        in_specs=(P("rep", None, None),) * 2 + (P("pp", None, None),) * 3,
        out_specs=(P(("rep", "pp"), None, None),) * 3,
        check_vma=False,
    )
```

```python
import jax
import jax.numpy as jnp
from jax import lax
from jax.experimental import pallas as pl
from jax.experimental.pallas import tpu as pltpu
from jax.sharding import PartitionSpec as P

F32, BF16 = jnp.float32, jnp.bfloat16
EPS = 1e-6
DOWN = 352
Q = 128
COARSE_F, COARSE_B, FINE = 256, 256, 128
AHEAD = (13, 12, 10, 9, 5, 4, 2, 0)
FINE_F = 6
FINE_B = 2
FINE_E = 8
RELAY_F, RELAY_B = 0, 7
LAG_F = 2
LAG_B = 3
FROM_F = 3
UPTO_B = 8


def dot(a, b):
    return jnp.dot(a, b, preferred_element_type=F32)


def kernel(
    x, dy, w_gate, w_up, w_down, o_gate, o_up, o_down, kept_pq, kept_hid,
    f_in, b_in, r_in, f_out, b_out, w_both, w_d, wt_d, wt_g, wt_u, acc_both, acc_d, a_t, hid_t, d_both, pq_out, hid_out, pq_in, hid_in,
    f_recv, b_recv, r_recv, f_send, b_send, r_send, w_sem, o_sem, out_sem, in_sem,
):
    micro, tokens, d = x.shape
    ff = w_down.shape[0]
    quarters = tokens // Q
    blocks = ff // 128
    me = lax.axis_index("pp")
    stages = 8
    first, last = me == 0, me == stages - 1

    def w_copies():
        for j in range(blocks):
            src = pl.ds(128 * j, 128)
            yield pltpu.make_async_copy(w_gate.at[:, src], w_both.at[:, pl.ds(256 * j, 128)], w_sem.at[0, j])
            yield pltpu.make_async_copy(w_up.at[:, src], w_both.at[:, pl.ds(256 * j + 128, 128)], w_sem.at[1, j])
        yield pltpu.make_async_copy(w_down, w_d, w_sem.at[0, blocks])

    def rows(q, n=Q):
        return pl.ds(pl.multiple_of(q * Q, Q), n)

    def f_copy(m, q, to=None):
        to = jnp.minimum(me + 1, stages - 1) if to is None else to
        return pltpu.make_async_remote_copy(
            f_out.at[m % 2, rows(q)], f_in.at[m, rows(q)], f_send.at[m % 2, q], f_recv.at[m, q], device_id={"pp": to}
        )

    def b_copy(m, q, to=None):
        to = jnp.maximum(me - 1, 0) if to is None else to
        return pltpu.make_async_remote_copy(
            b_out.at[m % 2, rows(q)], b_in.at[m, rows(q)], b_send.at[m % 2, q], b_recv.at[m, q], device_id={"pp": to}
        )

    def f_by_relay(m, q):
        return pltpu.make_async_remote_copy(
            f_out.at[m % 2, rows(q)], r_in.at[m, q // 2], f_send.at[m % 2, q], r_recv.at[m, q // 2], device_id={"pp": RELAY_F}
        )

    def b_by_relay(m, q):
        return pltpu.make_async_remote_copy(
            b_out.at[m % 2, rows(q)], r_in.at[m, q // 2], b_send.at[m % 2, q], r_recv.at[m, q // 2], device_id={"pp": RELAY_B}
        )

    def f_relay(m, q):
        return pltpu.make_async_remote_copy(
            r_in.at[m, q // 2], f_in.at[m, rows(q)], r_send.at[m, q // 2], f_recv.at[m, q], device_id={"pp": 4}
        )

    def b_relay(m, q):
        return pltpu.make_async_remote_copy(
            r_in.at[m, q // 2], b_in.at[m, rows(q)], r_send.at[m, q // 2], b_recv.at[m, q], device_id={"pp": 3}
        )

    def send(m, q, nq, relayed, copy, by_relay):
        for k in range(nq):

            @pl.when(relayed & ((q + k) % 2 == 0))
            def _():
                by_relay(m, q + k).start()

            @pl.when(~relayed | ((q + k) % 2 == 1))
            def _():
                copy(m, q + k).start()

    def kept_out(m, q):
        return (
            pltpu.make_async_copy(pq_out.at[rows(q)], kept_pq.at[m, rows(q)], out_sem.at[0, q]),
            pltpu.make_async_copy(hid_out.at[rows(q)], kept_hid.at[m, rows(q)], out_sem.at[1, q]),
        )

    def kept_in(m, q):
        return (
            pltpu.make_async_copy(kept_pq.at[m, rows(q)], pq_in.at[rows(q)], in_sem.at[0, q]),
            pltpu.make_async_copy(kept_hid.at[m, rows(q)], hid_in.at[rows(q)], in_sem.at[1, q]),
        )

    for copy in w_copies():
        copy.start()

    def each(body, start, stop):
        @pl.loop(start, stop)
        def _(m):
            @pl.loop(0, quarters)
            def _(q):
                body(m, q)

    def load(start, stop):
        @pl.when(first)
        def _():
            each(lambda m, q: pltpu.make_async_copy(x.at[m, rows(q)], f_in.at[m, rows(q)], f_recv.at[m, q]).start(), start, stop)

        @pl.when(last)
        def _():
            each(lambda m, q: pltpu.make_async_copy(dy.at[m, rows(q)], b_in.at[m, rows(q)], b_recv.at[m, q]).start(), start, stop)

    load(0, 1)
    barrier = pltpu.get_barrier_semaphore()
    for other in range(1, stages):
        pl.semaphore_signal(barrier, inc=1, device_id={"pp": lax.rem(me + other, stages)})
    acc_both[...] = jnp.zeros_like(acc_both)
    acc_d[...] = jnp.zeros_like(acc_d)
    pl.semaphore_wait(barrier, stages - 1)

    for copy in w_copies():
        copy.wait()
    load(1, micro)

    def scale_of(wide):
        return lax.rsqrt(jnp.mean(wide * wide, -1, keepdims=True) + EPS)

    def gates(both):
        gate, up = both[:, :128], both[:, 128:]
        sig = jax.nn.sigmoid(gate)
        silu = gate * sig
        return silu, up * (sig + silu * (1 - sig)), (silu * up).astype(BF16)

    def forward(m, q, n):
        nq = n // Q
        for k in range(nq):
            f_copy(m, q + k).wait_recv()

        @pl.when(m >= 1)
        def _():
            for k in range(nq):
                for copy in kept_out(m - 1, q + k):
                    copy.wait()

        @pl.when(m >= 2)
        def _():
            for k in range(nq):
                f_copy(m - 2, q + k).wait_send()

        here = rows(q, n)
        h = f_in[m, here]
        wide = h.astype(F32)
        a = (wide * scale_of(wide)).astype(BF16)
        for j in range(blocks):
            silu, by_gate, hid = gates(dot(a, w_both[:, 256 * j : 256 * j + 256]))
            pq_out[here, 256 * j : 256 * j + 128] = silu
            pq_out[here, 256 * j + 128 : 256 * j + 256] = by_gate
            hid_out[here, 128 * j : 128 * j + 128] = hid
        f_out[m % 2, here] = h + dot(hid_out[here], w_d[...]).astype(BF16)
        send(m, q, nq, (me == 3) & (m >= FROM_F), f_copy, f_by_relay)
        for k in range(nq):
            for copy in kept_out(m, q + k):
                copy.start()

    def send_back(m, q, n):
        nq = n // Q

        @pl.when(m >= 2)
        def _():
            for k in range(nq):
                b_copy(m - 2, q + k).wait_send()

        here = rows(q, n)
        wide = f_in[m, here].astype(F32)
        scale = scale_of(wide)
        by_a = (dot(d_both[here, :ff], wt_g[...]).astype(BF16) + dot(d_both[here, ff:], wt_u[...]).astype(BF16)).astype(F32)
        by_scale = jnp.sum(by_a * wide, -1, keepdims=True)
        by_wide = by_a * scale - wide * (by_scale * scale * scale * scale * (1.0 / d))
        b_out[m % 2, here] = b_in[m, here] + by_wide.astype(BF16)
        send(m, q, nq, (me == 4) & (m < UPTO_B), b_copy, b_by_relay)

    def backward_last(m, q, n):
        for k in range(n // Q):
            b_copy(m, q + k).wait_recv()
            f_copy(m, q + k).wait_recv()
        here = rows(q, n)
        by_y = b_in[m, here]
        wide = f_in[m, here].astype(F32)
        a = (wide * scale_of(wide)).astype(BF16)
        a_t[:, here] = a.T
        for j in range(0, blocks, 2):
            c = min(2, blocks - j)
            by_hid = dot(by_y, wt_d[:, 128 * j : 128 * (j + c)]).astype(BF16).astype(F32)
            for k in range(j, j + c):
                silu, by_gate, hid = gates(dot(a, w_both[:, 256 * k : 256 * k + 256]))
                by = by_hid[:, 128 * (k - j) : 128 * (k - j) + 128]
                hid_t[128 * k : 128 * k + 128, here] = hid.T
                d_both[here, 128 * k : 128 * k + 128] = (by * by_gate).astype(BF16)
                d_both[here, ff + 128 * k : ff + 128 * k + 128] = (by * silu).astype(BF16)
        send_back(m, q, n)

    def backward(m, q, n):
        nq = n // Q
        for k in range(nq):
            ahead_m, ahead_q = m + (q + k + 2) // quarters, (q + k + 2) % quarters

            @pl.when(ahead_m < micro)
            def _():
                for copy in kept_in(ahead_m, ahead_q):
                    copy.start()

        for k in range(nq):
            for copy in kept_in(m, q + k):
                copy.wait()
            b_copy(m, q + k).wait_recv()
        here = rows(q, n)
        by_y = b_in[m, here]
        wide = f_in[m, here].astype(F32)
        a_t[:, here] = (wide * scale_of(wide)).astype(BF16).T
        hid_t[:, here] = hid_in[here].T
        for j in range(0, blocks, 2):
            c = min(2, blocks - j)
            by_hid = dot(by_y, wt_d[:, 128 * j : 128 * (j + c)]).astype(BF16).astype(F32)
            for k in range(j, j + c):
                by = by_hid[:, 128 * (k - j) : 128 * (k - j) + 128]
                d_both[here, 128 * k : 128 * k + 128] = (by * pq_in[here, 256 * k + 128 : 256 * k + 256]).astype(BF16)
                d_both[here, ff + 128 * k : ff + 128 * k + 128] = (by * pq_in[here, 256 * k : 256 * k + 128]).astype(BF16)

        @pl.when(~first)
        def _():
            send_back(m, q, n)

    def by_weights(m):
        for j in range(blocks):
            cols = slice(256 * j, 256 * j + 256)
            acc_both[:, cols] += dot(a_t[...], d_both[:, cols]).astype(BF16).astype(F32)
        by_y = b_in[m]
        for j in range(0, ff, DOWN):
            acc_d[j : j + DOWN, :] += dot(hid_t[j : j + DOWN, :], by_y).astype(BF16).astype(F32)

    def out_copies():
        for j in range(0, ff, DOWN):
            yield pltpu.make_async_copy(hid_t.at[pl.ds(j, DOWN)], o_down.at[pl.ds(j, DOWN)], o_sem.at[j // DOWN])
        for j in range(2 * blocks):
            to = o_gate if j < blocks else o_up
            yield pltpu.make_async_copy(d_both.at[:, pl.ds(128 * j, 128)], to.at[:, pl.ds(128 * (j % blocks), 128)], o_sem.at[8 + j])

    def last_by_weights(m):
        by_y = b_in[m]
        copies = list(out_copies())
        for j in range(0, ff, DOWN):
            total = acc_d[j : j + DOWN, :] + dot(hid_t[j : j + DOWN, :], by_y).astype(BF16).astype(F32)
            hid_t[j : j + DOWN, :] = total.astype(BF16)
        for copy in copies[: ff // DOWN]:
            copy.start()
        for half in range(2):
            mine = range(half * (blocks // 2), blocks if half else blocks // 2)
            for j in mine:
                cols = slice(256 * j, 256 * j + 256)
                total = acc_both[:, cols] + dot(a_t[...], d_both[:, cols]).astype(BF16).astype(F32)
                d_both[:, cols] = total.astype(BF16)
            for j in mine:
                for copy in copies[ff // DOWN + 2 * j : ff // DOWN + 2 * j + 2]:
                    copy.start()
        for copy in copies:
            copy.wait()

    def in_chunks(body, m, fine, coarse):
        for n, which in ((FINE, fine), (coarse, ~fine)):

            @pl.when(which)
            def _():
                @pl.loop(0, tokens // n)
                def _(p):
                    body(m, p * (n // Q), n)

    def transpose_weights():
        @pl.loop(0, blocks)
        def _(j):
            cols = pl.ds(pl.multiple_of(128 * j, 128), 128)
            wt_d[:, cols] = w_d[cols, :].T
            wt_g[cols, :] = w_both[:, pl.ds(pl.multiple_of(256 * j, 128), 128)].T
            wt_u[cols, :] = w_both[:, pl.ds(pl.multiple_of(256 * j + 128, 128), 128)].T

    @pl.when(~first)
    def _():
        transpose_weights()

    ahead = jnp.int32(0)
    for s, k in enumerate(AHEAD):
        ahead = jnp.where(me == s, k, ahead)

    @pl.loop(0, micro + max(AHEAD))
    def _(i):
        @pl.when((i < micro) & ~last)
        def _():
            in_chunks(forward, i, i < FINE_F, COARSE_F)

        @pl.when((i == 0) & first)
        def _():
            transpose_weights()

        @pl.when((i == micro) & ~last)
        def _():
            for q in range(quarters):
                for copy in kept_out(micro - 1, q):
                    copy.wait()

        @pl.when((i == ahead - 1) & ~last)
        def _():
            for q in range(2):
                for copy in kept_in(0, q):
                    copy.start()

        for device, lag, arrives, relay, start, stop in (
            (RELAY_F, LAG_F, f_by_relay, f_relay, FROM_F, micro),
            (RELAY_B, LAG_B, b_by_relay, b_relay, 0, UPTO_B),
        ):

            @pl.when((me == device) & (i >= start + lag) & (i < stop + lag))
            def _():
                for q in range(0, quarters, 2):
                    arrives(i - lag, q).wait_recv()
                    relay(i - lag, q).start()

        m = i - ahead

        @pl.when((m >= 0) & (m < micro))
        def _():
            fine = (m < FINE_B) | (m >= micro - FINE_E)

            @pl.when(last)
            def _():
                in_chunks(backward_last, m, fine, COARSE_B)

            @pl.when(~last)
            def _():
                in_chunks(backward, m, fine, COARSE_B)

            @pl.when(m < micro - 1)
            def _():
                by_weights(m)

    for m in range(micro - 2, micro):
        for q in range(quarters):

            @pl.when(~last)
            def _():
                f_copy(m, q).wait_send()

            @pl.when(~first)
            def _():
                b_copy(m, q).wait_send()

    for device, relay, start, stop in ((RELAY_F, f_relay, FROM_F, micro), (RELAY_B, b_relay, 0, UPTO_B)):

        @pl.when(me == device)
        def _():
            @pl.loop(start, stop)
            def _(m):
                for q in range(0, quarters, 2):
                    relay(m, q).wait_send()

    last_by_weights(micro - 1)


def solution(mesh):
    def step(x, dy, w_gate, w_up, w_down):
        micro, tokens, d = x.shape
        ff = w_down.shape[1]
        quarters = tokens // Q
        hbm = pl.BlockSpec(memory_space=pl.ANY)
        dma = pltpu.SemaphoreType.DMA
        outs = pl.pallas_call(
            kernel,
            out_shape=(
                *(jax.ShapeDtypeStruct(w.shape[1:], w.dtype) for w in (w_gate, w_up, w_down)),
                jax.ShapeDtypeStruct((micro, tokens, 2 * ff), F32),
                jax.ShapeDtypeStruct((micro, tokens, ff), BF16),
            ),
            in_specs=[hbm] * 5,
            out_specs=(hbm,) * 5,
            scratch_shapes=[
                pltpu.VMEM((micro, tokens, d), BF16),
                pltpu.VMEM((micro, tokens, d), BF16),
                pltpu.VMEM((micro, quarters // 2, Q, d), BF16),
                pltpu.VMEM((2, tokens, d), BF16),
                pltpu.VMEM((2, tokens, d), BF16),
                pltpu.VMEM((d, 2 * ff), BF16),
                pltpu.VMEM((ff, d), BF16),
                pltpu.VMEM((d, ff), BF16),
                pltpu.VMEM((ff, d), BF16),
                pltpu.VMEM((ff, d), BF16),
                pltpu.VMEM((d, 2 * ff), F32),
                pltpu.VMEM((ff, d), F32),
                pltpu.VMEM((d, tokens), BF16),
                pltpu.VMEM((ff, tokens), BF16),
                pltpu.VMEM((tokens, 2 * ff), BF16),
                pltpu.VMEM((tokens, 2 * ff), F32),
                pltpu.VMEM((tokens, ff), BF16),
                pltpu.VMEM((tokens, 2 * ff), F32),
                pltpu.VMEM((tokens, ff), BF16),
                dma((micro, quarters)),
                dma((micro, quarters)),
                dma((micro, quarters // 2)),
                dma((2, quarters)),
                dma((2, quarters)),
                dma((micro, quarters // 2)),
                dma((2, ff // 128 + 1)),
                dma((8 + 2 * ff // 128,)),
                dma((2, quarters)),
                dma((2, quarters)),
            ],
            compiler_params=pltpu.CompilerParams(
                collective_id=0, has_side_effects=True, vmem_limit_bytes=67_043_328
            ),
        )(x, dy, w_gate[0], w_up[0], w_down[0])
        return tuple(o[None] for o in outs[:3])

    return jax.shard_map(
        step,
        mesh=mesh,
        in_specs=(P("rep", None, None),) * 2 + (P("pp", None, None),) * 3,
        out_specs=(P(("rep", "pp"), None, None),) * 3,
        check_vma=False,
    )
```

```python
import jax
import jax.numpy as jnp
from jax import lax
from jax.experimental import pallas as pl
from jax.experimental.pallas import tpu as pltpu
from jax.sharding import PartitionSpec as P

F32, BF16 = jnp.float32, jnp.bfloat16
EPS = 1e-6
DOWN = 352
Q = 128
COARSE_F, COARSE_B, FINE = 256, 256, 128
AHEAD = (13, 12, 9, 8, 5, 4, 2, 0)
FINE_F = 8
FINE_B = 2
FINE_E = 6
RELAY_F, RELAY_B = 0, 7
LAG_F = 2
LAG_B = 3
FROM_F = 3
UPTO_B = 8


def dot(a, b):
    return jnp.dot(a, b, preferred_element_type=F32)


def kernel(
    x, dy, w_gate, w_up, w_down, o_gate, o_up, o_down, kept_pq, kept_hid,
    f_in, b_in, r_in, f_out, b_out, w_both, w_d, wt_d, wt_g, wt_u, acc_both, acc_d, a_t, hid_t, d_both, pq_out, hid_out, pq_in, hid_in,
    f_recv, b_recv, r_recv, f_send, b_send, r_send, w_sem, o_sem, out_sem, in_sem,
):
    micro, tokens, d = x.shape
    ff = w_down.shape[0]
    quarters = tokens // Q
    blocks = ff // 128
    me = lax.axis_index("pp")
    stages = 8
    first, last = me == 0, me == stages - 1

    def w_copies():
        for j in range(blocks):
            src = pl.ds(128 * j, 128)
            yield pltpu.make_async_copy(w_gate.at[:, src], w_both.at[:, pl.ds(256 * j, 128)], w_sem.at[0, j])
            yield pltpu.make_async_copy(w_up.at[:, src], w_both.at[:, pl.ds(256 * j + 128, 128)], w_sem.at[1, j])
        yield pltpu.make_async_copy(w_down, w_d, w_sem.at[0, blocks])

    def rows(q, n=Q):
        return pl.ds(pl.multiple_of(q * Q, Q), n)

    def f_copy(m, q, to=None):
        to = jnp.minimum(me + 1, stages - 1) if to is None else to
        return pltpu.make_async_remote_copy(
            f_out.at[m % 2, rows(q)], f_in.at[m, rows(q)], f_send.at[m % 2, q], f_recv.at[m, q], device_id={"pp": to}
        )

    def b_copy(m, q, to=None):
        to = jnp.maximum(me - 1, 0) if to is None else to
        return pltpu.make_async_remote_copy(
            b_out.at[m % 2, rows(q)], b_in.at[m, rows(q)], b_send.at[m % 2, q], b_recv.at[m, q], device_id={"pp": to}
        )

    def f_by_relay(m, q):
        return pltpu.make_async_remote_copy(
            f_out.at[m % 2, rows(q)], r_in.at[m, q // 2], f_send.at[m % 2, q], r_recv.at[m, q // 2], device_id={"pp": RELAY_F}
        )

    def b_by_relay(m, q):
        return pltpu.make_async_remote_copy(
            b_out.at[m % 2, rows(q)], r_in.at[m, q // 2], b_send.at[m % 2, q], r_recv.at[m, q // 2], device_id={"pp": RELAY_B}
        )

    def f_relay(m, q):
        return pltpu.make_async_remote_copy(
            r_in.at[m, q // 2], f_in.at[m, rows(q)], r_send.at[m, q // 2], f_recv.at[m, q], device_id={"pp": 4}
        )

    def b_relay(m, q):
        return pltpu.make_async_remote_copy(
            r_in.at[m, q // 2], b_in.at[m, rows(q)], r_send.at[m, q // 2], b_recv.at[m, q], device_id={"pp": 3}
        )

    def send(m, q, nq, relayed, copy, by_relay):
        for k in range(nq):

            @pl.when(relayed & ((q + k) % 2 == 0))
            def _():
                by_relay(m, q + k).start()

            @pl.when(~relayed | ((q + k) % 2 == 1))
            def _():
                copy(m, q + k).start()

    def kept_out(m, q):
        return (
            pltpu.make_async_copy(pq_out.at[rows(q)], kept_pq.at[m, rows(q)], out_sem.at[0, q]),
            pltpu.make_async_copy(hid_out.at[rows(q)], kept_hid.at[m, rows(q)], out_sem.at[1, q]),
        )

    def kept_in(m, q):
        return (
            pltpu.make_async_copy(kept_pq.at[m, rows(q)], pq_in.at[rows(q)], in_sem.at[0, q]),
            pltpu.make_async_copy(kept_hid.at[m, rows(q)], hid_in.at[rows(q)], in_sem.at[1, q]),
        )

    for copy in w_copies():
        copy.start()

    def each(body, start, stop):
        @pl.loop(start, stop)
        def _(m):
            @pl.loop(0, quarters)
            def _(q):
                body(m, q)

    def load(start, stop):
        @pl.when(first)
        def _():
            each(lambda m, q: pltpu.make_async_copy(x.at[m, rows(q)], f_in.at[m, rows(q)], f_recv.at[m, q]).start(), start, stop)

        @pl.when(last)
        def _():
            each(lambda m, q: pltpu.make_async_copy(dy.at[m, rows(q)], b_in.at[m, rows(q)], b_recv.at[m, q]).start(), start, stop)

    load(0, 1)
    barrier = pltpu.get_barrier_semaphore()
    for other in range(1, stages):
        pl.semaphore_signal(barrier, inc=1, device_id={"pp": lax.rem(me + other, stages)})
    acc_both[...] = jnp.zeros_like(acc_both)
    acc_d[...] = jnp.zeros_like(acc_d)
    pl.semaphore_wait(barrier, stages - 1)

    for copy in w_copies():
        copy.wait()
    load(1, micro)

    def scale_of(wide):
        return lax.rsqrt(jnp.mean(wide * wide, -1, keepdims=True) + EPS)

    def gates(both):
        gate, up = both[:, :128], both[:, 128:]
        sig = jax.nn.sigmoid(gate)
        silu = gate * sig
        return silu, up * (sig + silu * (1 - sig)), (silu * up).astype(BF16)

    def forward(m, q, n):
        nq = n // Q
        for k in range(nq):
            f_copy(m, q + k).wait_recv()

        @pl.when(m >= 1)
        def _():
            for k in range(nq):
                for copy in kept_out(m - 1, q + k):
                    copy.wait()

        @pl.when(m >= 2)
        def _():
            for k in range(nq):
                f_copy(m - 2, q + k).wait_send()

        here = rows(q, n)
        h = f_in[m, here]
        wide = h.astype(F32)
        a = (wide * scale_of(wide)).astype(BF16)
        for j in range(blocks):
            silu, by_gate, hid = gates(dot(a, w_both[:, 256 * j : 256 * j + 256]))
            pq_out[here, 256 * j : 256 * j + 128] = silu
            pq_out[here, 256 * j + 128 : 256 * j + 256] = by_gate
            hid_out[here, 128 * j : 128 * j + 128] = hid
        f_out[m % 2, here] = h + dot(hid_out[here], w_d[...]).astype(BF16)
        send(m, q, nq, (me == 3) & (m >= FROM_F), f_copy, f_by_relay)
        for k in range(nq):
            for copy in kept_out(m, q + k):
                copy.start()

    def send_back(m, q, n):
        nq = n // Q

        @pl.when(m >= 2)
        def _():
            for k in range(nq):
                b_copy(m - 2, q + k).wait_send()

        here = rows(q, n)
        wide = f_in[m, here].astype(F32)
        scale = scale_of(wide)
        by_a = (dot(d_both[here, :ff], wt_g[...]).astype(BF16) + dot(d_both[here, ff:], wt_u[...]).astype(BF16)).astype(F32)
        by_scale = jnp.sum(by_a * wide, -1, keepdims=True)
        by_wide = by_a * scale - wide * (by_scale * scale * scale * scale * (1.0 / d))
        b_out[m % 2, here] = b_in[m, here] + by_wide.astype(BF16)
        send(m, q, nq, (me == 4) & (m < UPTO_B), b_copy, b_by_relay)

    def backward_last(m, q, n):
        for k in range(n // Q):
            b_copy(m, q + k).wait_recv()
            f_copy(m, q + k).wait_recv()
        here = rows(q, n)
        by_y = b_in[m, here]
        wide = f_in[m, here].astype(F32)
        a = (wide * scale_of(wide)).astype(BF16)
        a_t[:, here] = a.T
        for j in range(0, blocks, 2):
            c = min(2, blocks - j)
            by_hid = dot(by_y, wt_d[:, 128 * j : 128 * (j + c)]).astype(BF16).astype(F32)
            for k in range(j, j + c):
                silu, by_gate, hid = gates(dot(a, w_both[:, 256 * k : 256 * k + 256]))
                by = by_hid[:, 128 * (k - j) : 128 * (k - j) + 128]
                hid_t[128 * k : 128 * k + 128, here] = hid.T
                d_both[here, 128 * k : 128 * k + 128] = (by * by_gate).astype(BF16)
                d_both[here, ff + 128 * k : ff + 128 * k + 128] = (by * silu).astype(BF16)
        send_back(m, q, n)

    def backward(m, q, n):
        nq = n // Q
        for k in range(nq):
            ahead_m, ahead_q = m + (q + k + 2) // quarters, (q + k + 2) % quarters

            @pl.when(ahead_m < micro)
            def _():
                for copy in kept_in(ahead_m, ahead_q):
                    copy.start()

        for k in range(nq):
            for copy in kept_in(m, q + k):
                copy.wait()
            b_copy(m, q + k).wait_recv()
        here = rows(q, n)
        by_y = b_in[m, here]
        wide = f_in[m, here].astype(F32)
        a_t[:, here] = (wide * scale_of(wide)).astype(BF16).T
        hid_t[:, here] = hid_in[here].T
        for j in range(0, blocks, 2):
            c = min(2, blocks - j)
            by_hid = dot(by_y, wt_d[:, 128 * j : 128 * (j + c)]).astype(BF16).astype(F32)
            for k in range(j, j + c):
                by = by_hid[:, 128 * (k - j) : 128 * (k - j) + 128]
                d_both[here, 128 * k : 128 * k + 128] = (by * pq_in[here, 256 * k + 128 : 256 * k + 256]).astype(BF16)
                d_both[here, ff + 128 * k : ff + 128 * k + 128] = (by * pq_in[here, 256 * k : 256 * k + 128]).astype(BF16)

        @pl.when(~first)
        def _():
            send_back(m, q, n)

    def by_weights(m):
        for j in range(blocks):
            cols = slice(256 * j, 256 * j + 256)
            acc_both[:, cols] += dot(a_t[...], d_both[:, cols]).astype(BF16).astype(F32)
        by_y = b_in[m]
        for j in range(0, ff, DOWN):
            acc_d[j : j + DOWN, :] += dot(hid_t[j : j + DOWN, :], by_y).astype(BF16).astype(F32)

    def out_copies():
        for j in range(0, ff, DOWN):
            yield pltpu.make_async_copy(hid_t.at[pl.ds(j, DOWN)], o_down.at[pl.ds(j, DOWN)], o_sem.at[j // DOWN])
        for j in range(2 * blocks):
            to = o_gate if j < blocks else o_up
            yield pltpu.make_async_copy(d_both.at[:, pl.ds(128 * j, 128)], to.at[:, pl.ds(128 * (j % blocks), 128)], o_sem.at[8 + j])

    def last_by_weights(m):
        by_y = b_in[m]
        copies = list(out_copies())
        for j in range(0, ff, DOWN):
            total = acc_d[j : j + DOWN, :] + dot(hid_t[j : j + DOWN, :], by_y).astype(BF16).astype(F32)
            hid_t[j : j + DOWN, :] = total.astype(BF16)
        for copy in copies[: ff // DOWN]:
            copy.start()
        for half in range(2):
            mine = range(half * (blocks // 2), blocks if half else blocks // 2)
            for j in mine:
                cols = slice(256 * j, 256 * j + 256)
                total = acc_both[:, cols] + dot(a_t[...], d_both[:, cols]).astype(BF16).astype(F32)
                d_both[:, cols] = total.astype(BF16)
            for j in mine:
                for copy in copies[ff // DOWN + 2 * j : ff // DOWN + 2 * j + 2]:
                    copy.start()
        for copy in copies:
            copy.wait()

    def in_chunks(body, m, fine, coarse):
        for n, which in ((FINE, fine), (coarse, ~fine)):

            @pl.when(which)
            def _():
                @pl.loop(0, tokens // n)
                def _(p):
                    body(m, p * (n // Q), n)

    def transpose_weights():
        @pl.loop(0, blocks)
        def _(j):
            cols = pl.ds(pl.multiple_of(128 * j, 128), 128)
            wt_d[:, cols] = w_d[cols, :].T
            wt_g[cols, :] = w_both[:, pl.ds(pl.multiple_of(256 * j, 128), 128)].T
            wt_u[cols, :] = w_both[:, pl.ds(pl.multiple_of(256 * j + 128, 128), 128)].T

    @pl.when(~first)
    def _():
        transpose_weights()

    ahead = jnp.int32(0)
    for s, k in enumerate(AHEAD):
        ahead = jnp.where(me == s, k, ahead)

    @pl.loop(0, micro + max(AHEAD))
    def _(i):
        @pl.when((i < micro) & ~last)
        def _():
            in_chunks(forward, i, i < FINE_F, COARSE_F)

        @pl.when((i == 0) & first)
        def _():
            transpose_weights()

        @pl.when((i == micro) & ~last)
        def _():
            for q in range(quarters):
                for copy in kept_out(micro - 1, q):
                    copy.wait()

        @pl.when((i == ahead - 1) & ~last)
        def _():
            for q in range(2):
                for copy in kept_in(0, q):
                    copy.start()

        for device, lag, arrives, relay, start, stop in (
            (RELAY_F, LAG_F, f_by_relay, f_relay, FROM_F, micro),
            (RELAY_B, LAG_B, b_by_relay, b_relay, 0, UPTO_B),
        ):

            @pl.when((me == device) & (i >= start + lag) & (i < stop + lag))
            def _():
                for q in range(0, quarters, 2):
                    arrives(i - lag, q).wait_recv()
                    relay(i - lag, q).start()

        m = i - ahead

        @pl.when((m >= 0) & (m < micro))
        def _():
            fine = (m < FINE_B) | (m >= micro - FINE_E)

            @pl.when(last)
            def _():
                in_chunks(backward_last, m, fine, COARSE_B)

            @pl.when(~last)
            def _():
                in_chunks(backward, m, fine, COARSE_B)

            @pl.when(m < micro - 1)
            def _():
                by_weights(m)

    for m in range(micro - 2, micro):
        for q in range(quarters):

            @pl.when(~last)
            def _():
                f_copy(m, q).wait_send()

            @pl.when(~first)
            def _():
                b_copy(m, q).wait_send()

    for device, relay, start, stop in ((RELAY_F, f_relay, FROM_F, micro), (RELAY_B, b_relay, 0, UPTO_B)):

        @pl.when(me == device)
        def _():
            @pl.loop(start, stop)
            def _(m):
                for q in range(0, quarters, 2):
                    relay(m, q).wait_send()

    last_by_weights(micro - 1)


def solution(mesh):
    def step(x, dy, w_gate, w_up, w_down):
        micro, tokens, d = x.shape
        ff = w_down.shape[1]
        quarters = tokens // Q
        hbm = pl.BlockSpec(memory_space=pl.ANY)
        dma = pltpu.SemaphoreType.DMA
        outs = pl.pallas_call(
            kernel,
            out_shape=(
                *(jax.ShapeDtypeStruct(w.shape[1:], w.dtype) for w in (w_gate, w_up, w_down)),
                jax.ShapeDtypeStruct((micro, tokens, 2 * ff), F32),
                jax.ShapeDtypeStruct((micro, tokens, ff), BF16),
            ),
            in_specs=[hbm] * 5,
            out_specs=(hbm,) * 5,
            scratch_shapes=[
                pltpu.VMEM((micro, tokens, d), BF16),
                pltpu.VMEM((micro, tokens, d), BF16),
                pltpu.VMEM((micro, quarters // 2, Q, d), BF16),
                pltpu.VMEM((2, tokens, d), BF16),
                pltpu.VMEM((2, tokens, d), BF16),
                pltpu.VMEM((d, 2 * ff), BF16),
                pltpu.VMEM((ff, d), BF16),
                pltpu.VMEM((d, ff), BF16),
                pltpu.VMEM((ff, d), BF16),
                pltpu.VMEM((ff, d), BF16),
                pltpu.VMEM((d, 2 * ff), F32),
                pltpu.VMEM((ff, d), F32),
                pltpu.VMEM((d, tokens), BF16),
                pltpu.VMEM((ff, tokens), BF16),
                pltpu.VMEM((tokens, 2 * ff), BF16),
                pltpu.VMEM((tokens, 2 * ff), F32),
                pltpu.VMEM((tokens, ff), BF16),
                pltpu.VMEM((tokens, 2 * ff), F32),
                pltpu.VMEM((tokens, ff), BF16),
                dma((micro, quarters)),
                dma((micro, quarters)),
                dma((micro, quarters // 2)),
                dma((2, quarters)),
                dma((2, quarters)),
                dma((micro, quarters // 2)),
                dma((2, ff // 128 + 1)),
                dma((8 + 2 * ff // 128,)),
                dma((2, quarters)),
                dma((2, quarters)),
            ],
            compiler_params=pltpu.CompilerParams(
                collective_id=0, has_side_effects=True, vmem_limit_bytes=67_043_328
            ),
        )(x, dy, w_gate[0], w_up[0], w_down[0])
        return tuple(o[None] for o in outs[:3])

    return jax.shard_map(
        step,
        mesh=mesh,
        in_specs=(P("rep", None, None),) * 2 + (P("pp", None, None),) * 3,
        out_specs=(P(("rep", "pp"), None, None),) * 3,
        check_vma=False,
    )
```
